32 devices in a mesh: dp: 2 (over core), expert: 4 (over z), head: 4 (over y, x).
Axes of the slice: x: 2, y: 2, z: 4, core: 2. Of those that a mesh axis runs over, the one named last changes fastest.
Arguments:
- inputs: bfloat16 [4096, 1024], P(('dp', 'expert', 'head')), may hold values from -6 to 6
- cotangent: bfloat16 [4096, 1024], P(('dp', 'expert', 'head')), may hold values from -6 to 6
- segment_starts: int32 [4, 2], P('expert'), may hold values from 0 to 768, as said below
- routes: int32 [2, 4096, 8], P(None, ('dp', 'expert', 'head')), may hold values from 0 to 31, all different within a row; in each aligned block of 128 rows (0 to 127, 128 to 255, ..., all dimensions but the last counted through in order) at most 34 rows name the same one
- attention_gain: float32 [2, 1024], replicated, may hold values from 0.1 to 1.9
- mixture_gain: float32 [2, 1024], replicated, may hold values from 0.1 to 1.9
- query_weight: bfloat16 [2, 1024, 1024], P(None, 'expert', 'head'), may hold values from -0.1875 to 0.1875
- key_weight: bfloat16 [2, 1024, 512], P(None, 'expert', 'head'), may hold values from -0.1875 to 0.1875
- value_weight: bfloat16 [2, 1024, 512], P(None, 'expert', 'head'), may hold values from -0.1875 to 0.1875
- output_weight: bfloat16 [2, 1024, 1024], P(None, 'head', 'expert'), may hold values from -3 to 3
- router_weight: bfloat16 [2, 1024, 32], replicated, may hold values from -0.09375 to 0.09375
- expert_in: bfloat16 [2, 32, 1024, 1024], P(None, 'expert'), may hold values from -0.1875 to 0.1875
- expert_out: bfloat16 [2, 32, 512, 1024], P(None, 'expert'), may hold values from -0.75 to 0.75
Outputs:
- outputs: bfloat16 [4096, 1024], P(('dp', 'expert', 'head'))
- input_grad: float32 [4096, 1024], P(('dp', 'expert', 'head'))
- attention_gain_grad: float32 [2, 1024], replicated
- mixture_gain_grad: float32 [2, 1024], replicated
- query_grad: float32 [2, 1024, 1024], P(None, ('dp', 'expert'), 'head')
- key_grad: float32 [2, 1024, 512], P(None, ('dp', 'expert'), 'head')
- value_grad: float32 [2, 1024, 512], P(None, ('dp', 'expert'), 'head')
- output_grad: float32 [2, 1024, 1024], P(None, 'head', ('dp', 'expert'))
- router_grad: float32 [2, 1024, 32], replicated
- expert_in_grad: float32 [2, 32, 1024, 1024], P(None, 'expert', ('dp', 'head'))
- expert_out_grad: float32 [2, 32, 512, 1024], P(None, 'expert', ('dp', 'head'))
The draws below stay inside these ranges and needn't reach their ends.
Inputs may be any that keep to these rules, and one draw needn't show every extreme that they name: `routes`: each row names 8 different experts. Within each aligned block of 128 rows in one layer, no expert is named by more than 34 rows, a bound that some block reaches. `segment_starts`: A sequence's 2 segments of 256 positions lie inside it, disjoint and in rising order, the s-th within the s-th of 2 equal parts of the sequence. A start of 0 and a start of 768 occur in every draw.
All inputs are finite; a program needn't handle non-finite values.
Results may differ from the reference program's by a relative error of at most 0.03.
Values may be sent and summed in bfloat16 or wider, within the bound.
A program may use at most 320 MiB of HBM per device.

```python
import math
import jax
import jax.numpy as jnp
import numpy as np
from jax import lax

D = 1024
HEADS = 16
KV_HEADS = 8
HEAD_DIM = 64
FF = 512
EXPERTS = 32
TOP = 8
LAYERS = 2
BIDI = 256
NSEG = 2
TOK_DEV = 128
CAP = 34
SEQS = 4
TOKENS = 4096
N_DP = 2
N_HEAD = 4


def draw_segment_starts(key, part):
    length = TOK_DEV * N_HEAD * N_DP
    room = length // NSEG - BIDI + 1
    offsets = jax.random.randint(key, (SEQS, NSEG), 0, room)
    base = jnp.arange(NSEG, dtype=jnp.int32) * (length // NSEG)
    starts = base[None, :] + offsets.astype(jnp.int32)
    starts = starts.at[0, 0].set(0)
    starts = starts.at[0, NSEG - 1].set(length - BIDI)
    return starts.astype(jnp.int32)


def levels(key, dims, pieces, least, top_value):
    factor_of = 1.0
    for dim, blocks in pieces:
        steps = jax.random.uniform(jax.random.fold_in(jax.random.fold_in(key, 6), dim), (blocks,), jnp.float32, least / len(pieces), top_value / len(pieces))
        factor_of = factor_of * jnp.repeat(jnp.exp(steps), dims[dim] // blocks).reshape((-1,) + (1,) * (len(dims) - 1 - dim))
    return factor_of


def shared_out(key, own, number, rows, count, top, reach, lean):
    ranking = jax.random.permutation(key, count)
    packed, usual = load_shares(count, rows * top, reach, lean, True), load_shares(count, rows * top, reach, lean, False)
    places = jnp.arange(count)

    def named(tallies, offset_by):
        used = int((tallies > 0).sum())
        fixed = max(1, used // 4)
        shifted = fixed + (places - fixed + offset_by * (used - fixed)) % max(1, count - fixed)
        return jnp.zeros((count,), jnp.int32).at[ranking[jnp.where(places < fixed, places, shifted)]].set(jnp.asarray(tallies, jnp.int32))

    tallies = jnp.where(number % 4 == 0, named(packed, number // 4), named(usual, number - number // 4 - 1))
    mixed = jax.random.permutation(jax.random.fold_in(own, 3), count)
    giver, sink = mixed[0:count // 2 * 2:2], mixed[1:count // 2 * 2:2]
    room = jnp.minimum(tallies[giver] - 1, reach - tallies[sink]) // 2
    room = jnp.where((giver == ranking[0]) | (sink == ranking[0]) | (tallies[sink] == 0), 0, jnp.maximum(room, 0))
    shifted = jax.random.randint(jax.random.fold_in(own, 4), (count // 2,), 0, 1 << 20) % (room + 1)
    tallies = tallies.at[giver].add(-shifted).at[sink].add(shifted)
    items = jnp.searchsorted(jnp.cumsum(tallies), jnp.arange(rows * top), side="right").astype(jnp.int32)
    table = items.reshape(top, rows).T
    table = table[jax.random.permutation(jax.random.fold_in(own, 1), rows)]
    offset_by = jax.random.randint(jax.random.fold_in(own, 2), (rows, 1), 0, top)
    return jnp.take_along_axis(table, (jnp.arange(top)[None, :] + offset_by) % top, axis=1)


def load_shares(number_of, total, reach, skew, full):
    portions = [(1 << 20) // math.isqrt(grade ** skew) + 1 for grade in range(1, number_of + 1)]
    largest = reach if full else min(reach, max(-(-total // number_of), total * portions[0] // sum(portions)))
    least = 1 if total - largest >= number_of - 1 else 0
    counts, spare = [largest] + [least] * (number_of - 1), total - largest - least * (number_of - 1)
    while spare > 0:
        movable = [i for i in range(1, number_of) if counts[i] < largest] or [i for i in range(1, number_of) if counts[i] < reach]
        mass, remaining = sum([portions[i] for i in movable]), spare
        for i in movable:
            extra = min(reach - counts[i], max(1, remaining * portions[i] // mass), spare)
            counts[i] = counts[i] + extra
            spare = spare - extra
    return np.array(counts)


def gaussian(rng, shape, deviation, limit, split=(), kind=jnp.bfloat16):
    drawn = deviation * jax.random.normal(rng, shape, jnp.float32)
    if split:
        drawn = drawn * levels(rng, shape, split, -0.22, 0.18)
    return jnp.clip(drawn, -limit, limit).astype(kind)


def setup_inputs(seed: int = 0) -> dict:
    key_list = jax.random.split(jax.random.key(seed), 14)
    inputs = gaussian(key_list[0], (TOKENS, D), 1.0, 6.0, ((0, 32),))
    cotangent = gaussian(key_list[1], (TOKENS, D), 1.0, 6.0, ((0, 32),))
    segment_starts = draw_segment_starts(jax.random.fold_in(key_list[13], 71), 0)
    routes_keys = jax.random.split(jax.random.fold_in(key_list[3], 1), LAYERS * TOKENS // TOK_DEV)
    routes_turns = jax.random.permutation(jax.random.fold_in(key_list[3], 3), LAYERS * TOKENS // TOK_DEV)
    routes = jax.vmap(lambda own, number: shared_out(jax.random.fold_in(key_list[3], 2), own, number, TOK_DEV, EXPERTS, TOP, CAP, 2))(routes_keys, routes_turns).reshape((LAYERS, TOKENS, TOP))
    attention_gain = jnp.clip(1.0 + 0.18 * jax.random.normal(key_list[4], (LAYERS, D), jnp.float32), 0.1, 1.9)
    mixture_gain = jnp.clip(1.0 + 0.18 * jax.random.normal(key_list[5], (LAYERS, D), jnp.float32), 0.1, 1.9)
    query_weight = gaussian(key_list[6], (LAYERS, D, HEADS * HEAD_DIM), D ** -0.5, 0.1875, ((1, 4), (2, 4)))
    key_weight = gaussian(key_list[7], (LAYERS, D, KV_HEADS * HEAD_DIM), D ** -0.5, 0.1875, ((1, 4), (2, 4)))
    value_weight = gaussian(key_list[8], (LAYERS, D, KV_HEADS * HEAD_DIM), D ** -0.5, 0.1875, ((1, 4), (2, 4)))
    output_weight = gaussian(key_list[9], (LAYERS, HEADS * HEAD_DIM, D), (max(1, HEADS * HEAD_DIM // (TOK_DEV * N_HEAD * N_DP // 4))) ** -0.5, 3.0, ((1, 4), (2, 4)))
    router_weight = gaussian(key_list[10], (LAYERS, D, EXPERTS), (4 * D) ** -0.5, 0.09375)
    expert_in = gaussian(key_list[11], (LAYERS, EXPERTS, D, 2 * FF), D ** -0.5, 0.1875, ((1, 4),))
    expert_out = gaussian(key_list[12], (LAYERS, EXPERTS, FF, D), (FF // 8) ** -0.5, 0.75, ((1, 4),))
    return {"inputs": inputs, "cotangent": cotangent, "segment_starts": segment_starts, "routes": routes, "attention_gain": attention_gain, "mixture_gain": mixture_gain, "query_weight": query_weight, "key_weight": key_weight, "value_weight": value_weight, "output_weight": output_weight, "router_weight": router_weight, "expert_in": expert_in, "expert_out": expert_out}


EPS = 1e-06
THETA = 10000.0
NEG = -1e+30
HIGH = lax.Precision.HIGHEST

@jax.custom_vjp
def low(v):
    return lax.optimization_barrier(v.astype(jnp.bfloat16)).astype(jnp.float32)

@jax.custom_vjp
def low_back(v):
    return v

def low_keep(v):
    return (low(v), None)

def low_pass(kept, grad):
    return (grad,)

def back_keep(v):
    return (v, None)

def back_low(kept, grad):
    return (low(grad),)
low.defvjp(low_keep, low_pass)
low_back.defvjp(back_keep, back_low)

def rms_norm(values, gain):
    return values * lax.rsqrt(lax.optimization_barrier(jnp.mean(values * values, axis=-1, keepdims=True)) + EPS) * gain

def rotate(values, cosine, sine):
    half = values.shape[-1] // 2
    turned = jnp.concatenate([-values[..., half:], values[..., :half]], axis=-1)
    return values * cosine + turned * sine

def slot_positions(picks):
    hits = (picks[..., None] == jnp.arange(EXPERTS, dtype=jnp.int32)).astype(jnp.int32)
    before = jnp.cumsum(hits, axis=1) - hits
    return picks * CAP + lax.optimization_barrier(jnp.sum(before * hits, axis=-1))

def scatter_rows(slots, rows_in):
    return jnp.zeros((EXPERTS * CAP, rows_in.shape[-1]), jnp.float32).at[slots].set(rows_in)

def take_rows(table, slots):
    return table[slots]

def one_layer(params, layer, state, picks, mask, cosine, sine):
    attn_gain, moe_gain, query_w, key_w, value_w, output_w, router_w, expert_in_w, expert_out_w = [p[layer] for p in params]
    seqs, length, width = state.shape
    tokens = seqs * length
    share = HEADS // KV_HEADS
    h1 = low(rms_norm(state, attn_gain))
    queries = low_back(jnp.einsum('bld,de->ble', h1, query_w, precision=HIGH)).reshape(seqs, length, HEADS, HEAD_DIM)
    queries = low(rotate(queries, cosine, sine))
    keys = low_back(jnp.einsum('bld,de->ble', h1, key_w, precision=HIGH)).reshape(seqs, length, KV_HEADS, HEAD_DIM)
    keys = low(rotate(keys, cosine, sine))
    values = low(low_back(jnp.einsum('bld,de->ble', h1, value_w, precision=HIGH))).reshape(seqs, length, KV_HEADS, HEAD_DIM)
    keys = jnp.repeat(keys, share, axis=2)
    values = jnp.repeat(values, share, axis=2)
    scores = low_back(jnp.einsum('bqhd,bkhd->bhqk', queries, keys, precision=HIGH) * HEAD_DIM ** (-0.5))
    scores = jnp.where(mask[:, None], scores, NEG)
    probs = low(jax.nn.softmax(scores, axis=-1))
    heads_out = low(low_back(jnp.einsum('bhqk,bkhd->bqhd', probs, values, precision=HIGH)))
    attention = low_back(jnp.einsum('ble,ed->bld', heads_out.reshape(seqs, length, HEADS * HEAD_DIM), output_w, precision=HIGH))
    middle = (state + attention).reshape(tokens, width)
    h2 = low(rms_norm(middle, moe_gain))
    logits = jnp.dot(h2, router_w, precision=HIGH)
    gates = jax.nn.softmax(jnp.take_along_axis(logits, picks, axis=1), axis=-1)
    slot_of = slot_positions(picks.reshape(-1, TOK_DEV * TOP))
    blocks = slot_of.shape[0]
    copies = low_back(jnp.broadcast_to(h2[:, None, :], (tokens, TOP, width))).reshape(blocks, TOK_DEV * TOP, width)
    buffers = jax.vmap(scatter_rows)(slot_of, copies).reshape(blocks, EXPERTS, CAP, width)
    mixed = low_back(jnp.einsum('becd,edf->becf', buffers, expert_in_w, precision=HIGH))
    hidden = low(jax.nn.silu(mixed[..., :FF]) * mixed[..., FF:])
    expert_y = low(low_back(jnp.einsum('becf,efd->becd', hidden, expert_out_w, precision=HIGH)))
    expert_y = expert_y.reshape(blocks, EXPERTS * CAP, width)
    picked = jax.vmap(take_rows)(expert_y, slot_of).reshape(tokens, TOP, width)
    mixture = lax.optimization_barrier(jnp.sum(gates[..., None] * picked, axis=1))
    return (middle + mixture).reshape(seqs, length, width)

def two_layers(params, state, picks, starts):
    seqs, length, width = state.shape
    places = jnp.arange(length, dtype=jnp.int32)
    inside = (places[None, None, :] >= starts[:, :, None]) & (places[None, None, :] < starts[:, :, None] + BIDI)
    shared = jnp.any(inside[:, :, :, None] & inside[:, :, None, :], axis=1)
    mask = shared | (places[None, :] <= places[:, None])[None]
    half = HEAD_DIM // 2
    inverse = THETA ** (-(jnp.arange(half, dtype=jnp.float32) * 2.0 / HEAD_DIM))
    angle = places.astype(jnp.float32)[:, None] * inverse[None, :]
    angle = jnp.concatenate([angle, angle], axis=1)
    cosine = jnp.cos(angle)[:, None, :]
    sine = jnp.sin(angle)[:, None, :]
    for layer in range(LAYERS):
        state = one_layer(params, layer, state, picks[layer], mask, cosine, sine)
    return state

def to_sequences(array):
    piece = TOK_DEV * N_HEAD
    rest = array.shape[1:]
    shaped = array.reshape((N_DP, SEQS, piece) + rest)
    return jnp.swapaxes(shaped, 0, 1).reshape((SEQS * N_DP * piece,) + rest)

def from_sequences(array):
    piece = TOK_DEV * N_HEAD
    rest = array.shape[1:]
    shaped = array.reshape((SEQS, N_DP, piece) + rest)
    return jnp.swapaxes(shaped, 0, 1).reshape((TOKENS,) + rest)

def reference(inputs, cotangent, segment_starts, routes, attention_gain, mixture_gain, query_weight, key_weight, value_weight, output_weight, router_weight, expert_in, expert_out):
    length = TOK_DEV * N_HEAD * N_DP
    group = math.gcd(SEQS, max(1, 4096 // length))
    steps = SEQS // group
    params = tuple((p.astype(jnp.float32) for p in (attention_gain, mixture_gain, query_weight, key_weight, value_weight, output_weight, router_weight, expert_in, expert_out)))
    states = to_sequences(inputs.astype(jnp.float32)).reshape(steps, group, length, D)
    ordered = jnp.stack([to_sequences(routes[layer]) for layer in range(LAYERS)])
    picks = ordered.reshape(LAYERS, steps, group * length, TOP).transpose(1, 0, 2, 3)
    starts = segment_starts.reshape(steps, group, NSEG)
    checked = jax.checkpoint(two_layers)

    def run(weights, xs):

        def step(carry, item):
            state, pick, start = item
            return (carry, checked(weights, state, pick, start))
        unused, ys = lax.scan(step, jnp.zeros((), jnp.float32), (xs, picks, starts))
        return ys
    results, pull = jax.vjp(run, params, states)
    seeds = to_sequences(cotangent.astype(jnp.float32)).reshape(results.shape)
    grads, input_grad = pull(seeds)
    outputs = from_sequences(results.reshape(SEQS * length, D)).astype(jnp.bfloat16)
    back = from_sequences(input_grad.reshape(SEQS * length, D))
    return (outputs, back, grads[0], grads[1], grads[2], grads[3], grads[4], grads[5], grads[6], grads[7], grads[8])
```

```python
import functools

import jax
import jax.numpy as jnp
from jax import lax
from jax.experimental import pallas as pl
from jax.experimental.pallas import tpu as pltpu
from jax.sharding import PartitionSpec as P

MESH = pl.DeviceIdType.MESH

HEAD_DIM = 64
BIDI = 256
CAP = 34


EPS = 1e-06
THETA = 10000.0
NEG = -1e30
HIGH = lax.Precision.HIGHEST


def split_up(x, dim, devices):
    before, after = (x.shape[:dim], x.shape[dim + 1 :])
    return jnp.moveaxis(x.reshape(*before, devices, -1, *after), dim, 0)


def sum_at_owner(x, axis, dim):
    pieces = split_up(x, dim, lax.axis_size(axis))
    arrived = lax.all_to_all(pieces, axis, split_axis=0, concat_axis=0, tiled=True)
    return arrived.astype(jnp.float32).sum(axis=0)


def side_by_side(arrays, axis, dim, along):
    widths = [a.shape[along] for a in arrays]
    both = jnp.concatenate(arrays, axis=along)
    whole = sum_at_owner(both, axis, dim)
    return tuple(jnp.split(whole, [sum(widths[:k]) for k in range(1, len(widths))], axis=along))


def rms_scale(values):
    return lax.rsqrt(jnp.mean(values * values, axis=-1, keepdims=True) + EPS)


def norm_back(values, factor, gain, grad):
    normed = values * factor
    gain_grad = jnp.sum(grad * normed, axis=0)
    inner = grad * gain
    return (factor * (inner - normed * jnp.mean(inner * normed, axis=-1, keepdims=True)), gain_grad)


def rope_tables(places, head_dim):
    half = head_dim // 2
    inverse = THETA ** (-(jnp.arange(half, dtype=jnp.float32) * 2.0 / head_dim))
    angle = places.astype(jnp.float32)[:, None] * inverse[None, :]
    angle = jnp.concatenate([angle, angle], axis=1)
    return (jnp.cos(angle)[:, None, :], jnp.sin(angle)[:, None, :])


def rotate(values, cosine, sine, sign):
    half = values.shape[-1] // 2
    turned = jnp.concatenate([-values[..., half:], values[..., :half]], axis=-1)
    return values * cosine + sign * turned * sine


def visible(query_pos, key_pos, starts):
    causal = key_pos[None, :] <= query_pos[:, None]
    query_in = (query_pos[:, None] >= starts[None, :]) & (
        query_pos[:, None] < starts[None, :] + BIDI
    )
    key_in = (key_pos[:, None] >= starts[None, :]) & (key_pos[:, None] < starts[None, :] + BIDI)
    shared = jnp.any(query_in[:, None, :] & key_in[None, :, :], axis=-1)
    return causal | shared


def slot_tables(hits, capacity):
    picks_flat = jnp.argmax(hits, axis=1)
    before = jnp.cumsum(hits, axis=0) - hits
    slot = jnp.sum(before * hits, axis=1)
    slot_of = picks_flat * capacity + slot
    total = hits.shape[0]
    owner_of = (
        jnp.full((hits.shape[1] * capacity,), total, jnp.int32)
        .at[slot_of]
        .set(jnp.arange(total, dtype=jnp.int32))
    )
    return (slot_of, owner_of)


def contract_rows(left, right):
    return lax.dot_general(
        left, right, (((0,), (0,)), ((), ())), preferred_element_type=jnp.float32
    )


def contract_cols(left, right):
    return lax.dot_general(
        left, right, (((1,), (1,)), ((), ())), preferred_element_type=jnp.float32
    )


def per_device_rows(
    inputs,
    cotangent,
    segment_starts,
    routes,
    attention_gain,
    mixture_gain,
    query_weight,
    key_weight,
    value_weight,
    output_weight,
    router_weight,
    expert_in,
    expert_out,
):
    rows, width = inputs.shape
    half_len = rows * lax.axis_size("head")
    length = half_len * lax.axis_size("dp")
    block = min(512, half_len)
    nblocks = half_len // block
    head_dim = HEAD_DIM
    q_heads = query_weight.shape[2] // head_dim
    kv_heads = key_weight.shape[2] // head_dim
    share = q_heads // kv_heads
    layers = query_weight.shape[0]
    local_experts = expert_in.shape[1]
    owners = lax.axis_size("expert")
    all_experts = local_experts * owners
    capacity = CAP
    top = routes.shape[2]
    hidden_width = expert_out.shape[2]
    count = rows * top
    factor = head_dim ** (-0.5)
    offset = lax.axis_index("dp") * half_len
    positions = jnp.arange(length, dtype=jnp.int32)
    cosine, sine = rope_tables(positions, head_dim)
    cos_own = lax.dynamic_slice_in_dim(cosine, offset, half_len, 0)
    sin_own = lax.dynamic_slice_in_dim(sine, offset, half_len, 0)
    starts = segment_starts[0]
    block_ids = jnp.arange(nblocks, dtype=jnp.int32)
    expert_ids = jnp.arange(all_experts, dtype=jnp.int32)

    def block_scores(q_block, keys, index):
        query_pos = offset + index * block + jnp.arange(block, dtype=jnp.int32)
        mask = visible(query_pos, positions, starts)
        raw = (
            jnp.einsum("qcgd,kcd->cgqk", q_block, keys, preferred_element_type=jnp.float32) * factor
        )
        return jnp.where(mask[None, None], raw, NEG)

    current = inputs.astype(jnp.float32)
    saved = []
    for layer in range(layers):
        scale_one = rms_scale(current)
        normed_one = (current * scale_one * attention_gain[layer]).astype(jnp.bfloat16)
        full_rows = lax.all_gather(normed_one, ("dp", "head"), axis=0, tiled=True)
        own_rows = lax.dynamic_slice_in_dim(full_rows, offset, half_len, 0)
        weight_q, weight_k, weight_v, weight_o = (
            lax.all_gather(query_weight[layer], "expert", axis=0, tiled=True),
            lax.all_gather(key_weight[layer], "expert", axis=0, tiled=True),
            lax.all_gather(value_weight[layer], "expert", axis=0, tiled=True),
            lax.all_gather(output_weight[layer], "expert", axis=1, tiled=True),
        )
        query_lin = jnp.dot(own_rows, weight_q, preferred_element_type=jnp.float32).reshape(
            half_len, q_heads, head_dim
        )
        key_lin = jnp.dot(full_rows, weight_k, preferred_element_type=jnp.float32).reshape(
            length, kv_heads, head_dim
        )
        queries = rotate(query_lin, cos_own, sin_own, 1.0).astype(jnp.bfloat16)
        keys = rotate(key_lin, cosine, sine, 1.0).astype(jnp.bfloat16)
        values = (
            jnp.dot(full_rows, weight_v, preferred_element_type=jnp.float32)
            .astype(jnp.bfloat16)
            .reshape(length, kv_heads, head_dim)
        )
        grouped = queries.reshape(nblocks, block, kv_heads, share, head_dim)

        def attend(item):
            q_block, index = item
            scores = block_scores(q_block, keys, index)
            peak = jnp.max(scores, axis=-1, keepdims=True)
            weights = jnp.exp(scores - peak)
            total = jnp.sum(weights, axis=-1, keepdims=True)
            probs = (weights / total).astype(jnp.bfloat16)
            mixed_heads = jnp.einsum(
                "cgqk,kcd->qcgd", probs, values, preferred_element_type=jnp.float32
            )
            return (mixed_heads.astype(jnp.bfloat16), (peak + jnp.log(total))[..., 0])

        heads_out, log_totals = lax.map(attend, (grouped, block_ids))
        heads_flat = heads_out.reshape(half_len, q_heads * head_dim)
        summed = lax.psum(
            jnp.dot(heads_flat, weight_o, preferred_element_type=jnp.float32).astype(jnp.bfloat16),
            "head",
        ).astype(jnp.float32)
        attn_rows = lax.dynamic_slice_in_dim(summed, lax.axis_index("head") * rows, rows, 0)
        middle = current + attn_rows
        scale_two = rms_scale(middle)
        normed_two = (middle * scale_two * mixture_gain[layer]).astype(jnp.bfloat16)
        logits = jnp.dot(normed_two, router_weight[layer], preferred_element_type=jnp.float32)
        hits = routes[layer][:, :, None] == expert_ids[None, None, :]
        chosen = jnp.sum(jnp.where(hits, logits[:, None, :], 0.0), axis=-1)
        gates = jax.nn.softmax(chosen, axis=-1)
        slot_of, owner_of = slot_tables(
            hits.reshape(count, all_experts).astype(jnp.int32), capacity
        )
        valid = owner_of < count
        safe_owner = jnp.minimum(owner_of, count - 1)
        send = jnp.where(
            valid[:, None],
            jnp.take(normed_two, safe_owner // top, axis=0),
            jnp.zeros((), jnp.bfloat16),
        )
        send = send.reshape(owners, local_experts, capacity, width)
        received = lax.all_to_all(send, "expert", split_axis=0, concat_axis=0, tiled=True)
        mixed = jnp.einsum(
            "nerd,edf->nerf", received, expert_in[layer], preferred_element_type=jnp.float32
        )
        gate_part = mixed[..., :hidden_width]
        up_part = mixed[..., hidden_width:]
        hidden = (jax.nn.silu(gate_part) * up_part).astype(jnp.bfloat16)
        expert_y = jnp.einsum(
            "nerf,efd->nerd", hidden, expert_out[layer], preferred_element_type=jnp.float32
        ).astype(jnp.bfloat16)
        returned = lax.all_to_all(
            expert_y, "expert", split_axis=0, concat_axis=0, tiled=True
        ).reshape(all_experts * capacity, width)
        picked = jnp.take(returned, slot_of, axis=0).reshape(rows, top, width)
        after = middle + jnp.sum(gates[..., None] * picked, axis=1)
        saved.append(
            (
                current,
                scale_one,
                own_rows,
                weight_q,
                weight_k,
                weight_v,
                weight_o,
                grouped,
                keys,
                values,
                heads_flat,
                log_totals,
                middle,
                scale_two,
                normed_two,
                hits,
                gates,
                slot_of,
                valid,
                safe_owner,
                received,
                gate_part,
                up_part,
                hidden,
                picked,
            )
        )
        current = after
    outputs = current.astype(jnp.bfloat16)
    grad = cotangent.astype(jnp.float32)
    gain_a_list, gain_m_list, router_list = ([], [], [])
    query_list, key_list, value_list, out_list, in_list, down_list = ([], [], [], [], [], [])
    for layer in reversed(range(layers)):
        (
            state_in,
            scale_one,
            own_rows,
            weight_q,
            weight_k,
            weight_v,
            weight_o,
            grouped,
            keys,
            values,
            heads_flat,
            log_totals,
            middle,
            scale_two,
            normed_two,
            hits,
            gates,
            slot_of,
            valid,
            safe_owner,
            received,
            gate_part,
            up_part,
            hidden,
            picked,
        ) = saved[layer]
        dgates = jnp.sum(grad[:, None, :] * picked, axis=-1)
        dpicked = (gates[..., None] * grad[:, None, :]).astype(jnp.bfloat16).reshape(count, width)
        send_grad = jnp.where(
            valid[:, None], jnp.take(dpicked, safe_owner, axis=0), jnp.zeros((), jnp.bfloat16)
        )
        send_grad = send_grad.reshape(owners, local_experts, capacity, width)
        dexpert = lax.all_to_all(send_grad, "expert", split_axis=0, concat_axis=0, tiled=True)
        dhidden = jnp.einsum(
            "nerd,efd->nerf", dexpert, expert_out[layer], preferred_element_type=jnp.float32
        )
        grad_down = jnp.einsum(
            "nerf,nerd->efd", hidden, dexpert, preferred_element_type=jnp.float32
        )
        sigma = jax.nn.sigmoid(gate_part)
        dgate = dhidden * up_part * sigma * (1.0 + gate_part * (1.0 - sigma))
        dup = dhidden * (gate_part * sigma)
        dmixed = jnp.concatenate([dgate, dup], axis=-1).astype(jnp.bfloat16)
        grad_in_w = jnp.einsum(
            "nerd,nerf->edf", received, dmixed, preferred_element_type=jnp.float32
        )
        dinput_rows = jnp.einsum(
            "nerf,edf->nerd", dmixed, expert_in[layer], preferred_element_type=jnp.float32
        ).astype(jnp.bfloat16)
        dback = lax.all_to_all(
            dinput_rows, "expert", split_axis=0, concat_axis=0, tiled=True
        ).reshape(all_experts * capacity, width)
        dnormed_two = jnp.sum(
            jnp.take(dback, slot_of, axis=0).reshape(rows, top, width), axis=1, dtype=jnp.float32
        )
        dchosen = gates * (dgates - jnp.sum(gates * dgates, axis=-1, keepdims=True))
        dlogits = jnp.sum(jnp.where(hits, dchosen[..., None], 0.0), axis=1)
        dnormed_two = dnormed_two + jnp.dot(
            dlogits, router_weight[layer].astype(jnp.float32).T, precision=HIGH
        )
        router_list.insert(0, jnp.dot(normed_two.astype(jnp.float32).T, dlogits, precision=HIGH))
        dmiddle, gain_m = norm_back(middle, scale_two, mixture_gain[layer], dnormed_two)
        gain_m_list.insert(0, gain_m)
        dmiddle = grad + dmiddle
        full_dattn = lax.all_gather(dmiddle.astype(jnp.bfloat16), "head", axis=0, tiled=True)
        grad_o = contract_rows(heads_flat, full_dattn)
        dheads = contract_cols(full_dattn, weight_o).astype(jnp.bfloat16)
        dgrouped = dheads.reshape(nblocks, block, kv_heads, share, head_dim)

        def attend_back(carry, item):
            key_acc, value_acc = carry
            q_block, d_block, lse_block, index = item
            scores = block_scores(q_block, keys, index)
            probs = jnp.exp(scores - lse_block[..., None])
            dprobs = jnp.einsum(
                "qcgd,kcd->cgqk", d_block, values, preferred_element_type=jnp.float32
            )
            delta = jnp.sum(probs * dprobs, axis=-1, keepdims=True)
            dscores = (probs * (dprobs - delta)).astype(jnp.bfloat16)
            dquery = (
                jnp.einsum("cgqk,kcd->qcgd", dscores, keys, preferred_element_type=jnp.float32)
                * factor
            )
            key_acc = (
                key_acc
                + jnp.einsum("cgqk,qcgd->kcd", dscores, q_block, preferred_element_type=jnp.float32)
                * factor
            )
            value_acc = value_acc + jnp.einsum(
                "cgqk,qcgd->kcd",
                probs.astype(jnp.bfloat16),
                d_block,
                preferred_element_type=jnp.float32,
            )
            return ((key_acc, value_acc), dquery.reshape(block, q_heads, head_dim))

        empty = jnp.zeros((length, kv_heads, head_dim), jnp.float32)
        (dkeys_all, dvalues_all), dqueries = lax.scan(
            attend_back, (empty, empty), (grouped, dgrouped, log_totals, block_ids)
        )
        dkeys, dvalues = (
            lax.psum_scatter(
                dkeys_all.reshape(length, kv_heads * head_dim).astype(jnp.bfloat16),
                "dp",
                scatter_dimension=0,
                tiled=True,
            ).astype(jnp.float32),
            lax.psum_scatter(
                dvalues_all.reshape(length, kv_heads * head_dim).astype(jnp.bfloat16),
                "dp",
                scatter_dimension=0,
                tiled=True,
            ).astype(jnp.float32),
        )
        dquery_lin = (
            rotate(dqueries.reshape(half_len, q_heads, head_dim), cos_own, sin_own, -1.0)
            .astype(jnp.bfloat16)
            .reshape(half_len, q_heads * head_dim)
        )
        dkey_lin = (
            rotate(dkeys.reshape(half_len, kv_heads, head_dim), cos_own, sin_own, -1.0)
            .astype(jnp.bfloat16)
            .reshape(half_len, kv_heads * head_dim)
        )
        dvalue_lin = dvalues.astype(jnp.bfloat16)
        grad_q = contract_rows(own_rows, dquery_lin)
        grad_k = contract_rows(own_rows, dkey_lin)
        grad_v = contract_rows(own_rows, dvalue_lin)
        part_q = contract_cols(dquery_lin, weight_q)
        part_k = contract_cols(dkey_lin, weight_k)
        part_v = contract_cols(dvalue_lin, weight_v)
        dnormed_one = lax.psum_scatter(
            (part_q + part_k + part_v).astype(jnp.bfloat16), "head", scatter_dimension=0, tiled=True
        ).astype(jnp.float32)
        dstate, gain_a = norm_back(state_in, scale_one, attention_gain[layer], dnormed_one)
        gain_a_list.insert(0, gain_a)
        grad = dmiddle + dstate
        shard_q, shard_k, shard_v, shard_o = (
            *side_by_side(
                (
                    grad_q.astype(jnp.bfloat16),
                    grad_k.astype(jnp.bfloat16),
                    grad_v.astype(jnp.bfloat16),
                ),
                ("dp", "expert"),
                0,
                1,
            ),
            sum_at_owner(grad_o.astype(jnp.bfloat16), ("dp", "expert"), 1),
        )
        shard_in, shard_down = (
            lax.psum_scatter(
                grad_in_w.astype(jnp.bfloat16), ("dp", "head"), scatter_dimension=1, tiled=True
            ).astype(jnp.float32),
            lax.psum_scatter(
                grad_down.astype(jnp.bfloat16), ("dp", "head"), scatter_dimension=1, tiled=True
            ).astype(jnp.float32),
        )
        query_list.insert(0, shard_q)
        key_list.insert(0, shard_k)
        value_list.insert(0, shard_v)
        out_list.insert(0, shard_o)
        in_list.insert(0, shard_in)
        down_list.insert(0, shard_down)
    total_a, total_m, total_r = lax.psum(
        (jnp.stack(gain_a_list), jnp.stack(gain_m_list), jnp.stack(router_list)),
        ("dp", "expert", "head"),
    )
    return (
        outputs,
        grad,
        total_a,
        total_m,
        jnp.stack(query_list),
        jnp.stack(key_list),
        jnp.stack(value_list),
        jnp.stack(out_list),
        total_r,
        jnp.stack(in_list),
        jnp.stack(down_list),
    )


class Gather:
    def __init__(self, axis):
        self.axis = axis

    def out(self, x, sizes):
        return (sizes[self.axis],) + x.shape

    def axes(self):
        return (self.axis,)

    def sems(self, sizes):
        return sizes[self.axis] - 1, 1

    def start(self, x, o, send, recv, local, sizes):
        n, me = sizes[self.axis], lax.axis_index(self.axis)
        self.copies = []
        for k in range(1, n):
            self.copies.append(
                pltpu.make_async_remote_copy(
                    src_ref=x,
                    dst_ref=o.at[me],
                    send_sem=send.at[k - 1],
                    recv_sem=recv.at[k - 1],
                    device_id={self.axis: lax.rem(me + k, n)},
                    device_id_type=MESH,
                )
            )
        for copy in self.copies:
            copy.start()
        self.own = pltpu.make_async_copy(x, o.at[me], local.at[0])
        self.own.start()

    def relay(self):
        pass

    def finish(self):
        self.own.wait()
        for copy in self.copies:
            copy.wait()


class Exchange(Gather):
    def out(self, x, sizes):
        return x.shape

    def start(self, x, o, send, recv, local, sizes):
        n, me = sizes[self.axis], lax.axis_index(self.axis)
        self.copies = []
        for k in range(1, n):
            to = lax.rem(me + k, n)
            self.copies.append(
                pltpu.make_async_remote_copy(
                    src_ref=x.at[to],
                    dst_ref=o.at[me],
                    send_sem=send.at[k - 1],
                    recv_sem=recv.at[k - 1],
                    device_id={self.axis: to},
                    device_id_type=MESH,
                )
            )
        for copy in self.copies:
            copy.start()
        self.own = pltpu.make_async_copy(x.at[me], o.at[me], local.at[0])
        self.own.start()


class Spread:
    def __init__(self, shape=None, source=None, place=None):
        self.shape = shape
        self.source = source or (lambda x, d: x)
        self.place = place or (lambda o, d, z: o.at[d, z])

    def out(self, x, sizes):
        return self.shape or (sizes["dp"], sizes["expert"]) + x.shape

    def axes(self):
        return ("expert", "dp")

    def sems(self, sizes):
        return 2 * sizes["expert"] - 1, 1

    def start(self, x, o, send, recv, local, sizes):
        n, z, d = sizes["expert"], lax.axis_index("expert"), lax.axis_index("dp")
        mine, other = self.source(x, d), 1 - d
        self.copies, self.onward = [], []
        for k in range(1, n):
            self.copies.append(
                pltpu.make_async_remote_copy(
                    src_ref=mine,
                    dst_ref=self.place(o, d, z),
                    send_sem=send.at[k - 1],
                    recv_sem=recv.at[k - 1],
                    device_id={"expert": lax.rem(z + k, n)},
                    device_id_type=MESH,
                )
            )
        for k in range(n):
            origin = lax.rem(z - k + n, n)
            self.onward.append(
                pltpu.make_async_remote_copy(
                    src_ref=mine if k == 0 else self.place(o, d, origin),
                    dst_ref=self.place(o, d, origin),
                    send_sem=send.at[n - 1 + k],
                    recv_sem=recv.at[n - 1 + k],
                    device_id={"dp": other},
                    device_id_type=MESH,
                )
            )
        for copy in self.copies:
            copy.start()
        self.onward[0].start()
        self.own = pltpu.make_async_copy(mine, self.place(o, d, z), local.at[0])
        self.own.start()

    def relay(self):
        for k, copy in enumerate(self.copies):
            copy.wait_recv()
            self.onward[k + 1].start()

    def finish(self):
        self.own.wait()
        for copy in self.copies:
            copy.wait_send()
        for copy in self.onward:
            copy.wait()


class Swap:
    def out(self, x, sizes):
        return x.shape[1:]

    def axes(self):
        return ("dp",)

    def sems(self, sizes):
        return 1, 0

    def start(self, x, o, send, recv, local, sizes):
        other = 1 - lax.axis_index("dp")
        self.copy = pltpu.make_async_remote_copy(
            src_ref=x.at[other],
            dst_ref=o,
            send_sem=send.at[0],
            recv_sem=recv.at[0],
            device_id={"dp": other},
            device_id_type=MESH,
        )
        self.copy.start()

    def relay(self):
        pass

    def finish(self):
        self.copy.wait()


def transfer_body(makers, sizes, *refs):
    count = len(makers)
    ins, outs, sems = refs[:count], refs[count : 2 * count], refs[2 * count :]
    tasks = [make() for make in makers]
    axes = []
    for task in tasks:
        axes += [axis for axis in task.axes() if axis not in axes]
    barrier = pltpu.get_barrier_semaphore()
    greeted = 0
    for axis in axes:
        n, me = sizes[axis], lax.axis_index(axis)
        for k in range(1, n):
            pl.semaphore_signal(
                barrier, inc=1, device_id={axis: lax.rem(me + k, n)}, device_id_type=MESH
            )
            greeted += 1
    pl.semaphore_wait(barrier, greeted)
    for t, task in enumerate(tasks):
        task.start(ins[t], outs[t], *sems[3 * t : 3 * t + 3], sizes)
    for task in tasks:
        task.relay()
    for task in tasks:
        task.finish()


def transfer(name, number, makers, arrays):
    sizes = {axis: lax.axis_size(axis) for axis in ("dp", "expert", "head")}
    tasks = [make() for make in makers]
    scratch = []
    for task in tasks:
        remote, local = task.sems(sizes)
        scratch += [
            pltpu.SemaphoreType.DMA((remote,)),
            pltpu.SemaphoreType.DMA((remote,)),
            pltpu.SemaphoreType.DMA((max(1, local),)),
        ]
    vmem = pl.BlockSpec(memory_space=pltpu.VMEM)
    return pl.pallas_call(
        functools.partial(transfer_body, makers, sizes),
        out_shape=[
            jax.ShapeDtypeStruct(task.out(x, sizes), x.dtype) for task, x in zip(tasks, arrays)
        ],
        in_specs=[vmem] * len(arrays),
        out_specs=[vmem] * len(arrays),
        scratch_shapes=scratch,
        compiler_params=pltpu.CompilerParams(collective_id=number, has_side_effects=True),
        name=name,
    )(*arrays)


def token_plan_fits(mesh):
    return mesh.shape["dp"] == 2 and mesh.shape["expert"] <= 8


def per_device_dense(
    inputs,
    cotangent,
    segment_starts,
    routes,
    attention_gain,
    mixture_gain,
    query_weight,
    key_weight,
    value_weight,
    output_weight,
    router_weight,
    expert_in,
    expert_out,
):
    f32, bf16 = jnp.float32, jnp.bfloat16
    rows, width = inputs.shape
    cores, owners, heads_axis = (lax.axis_size(a) for a in ("dp", "expert", "head"))
    half_len = rows * heads_axis
    length = half_len * cores
    head_dim = HEAD_DIM
    q_width, kv_width = query_weight.shape[2], key_weight.shape[2]
    q_heads, kv_heads = q_width // head_dim, kv_width // head_dim
    share = q_heads // kv_heads
    layers = query_weight.shape[0]
    own_experts = expert_in.shape[1]
    per_core = own_experts // cores
    all_experts = own_experts * owners
    hidden_width = expert_out.shape[2]
    group = rows * cores * owners
    capacity = -(-cores * owners * CAP // 16) * 16
    factor = head_dim ** (-0.5)
    core, owner, place = (lax.axis_index(a) for a in ("dp", "expert", "head"))
    offset = core * half_len
    positions = jnp.arange(length, dtype=jnp.int32)
    own_positions = offset + jnp.arange(half_len, dtype=jnp.int32)
    cos_own, sin_own = rope_tables(own_positions, head_dim)
    mask = visible(own_positions, positions, segment_starts[0])
    first_expert = owner * own_experts + core * per_core

    def dot(left, right, dims):
        return lax.dot_general(left, right, (dims, ((), ())), preferred_element_type=f32)

    wide = q_width + 2 * kv_width
    piece = width // owners
    packed = jnp.concatenate([query_weight, key_weight, value_weight], axis=2)
    out_rows = output_weight.shape[1]

    def weight_tasks():
        return [
            lambda: Spread(
                (owners, cores, piece // cores, wide),
                lambda x, d: x.at[d],
                lambda o, d, z: o.at[z, d],
            ),
            lambda: Spread(
                (cores, out_rows // cores, width),
                lambda x, d: x.at[d],
                lambda o, d, z: o.at[d, :, pl.ds(pl.multiple_of(z * piece, piece), piece)],
            ),
        ]

    def weight_pieces(layer):
        return [
            packed[layer].reshape(cores, piece // cores, wide),
            output_weight[layer].reshape(cores, out_rows // cores, piece),
        ]

    def whole_weights(arrived):
        return arrived[0].reshape(width, wide), arrived[1].reshape(out_rows, width)

    lanes = -(-layers * all_experts // 128) * 128
    expert_ids = jnp.arange(all_experts, dtype=jnp.int32)
    named = jnp.any(routes[..., None] == expert_ids, axis=2).astype(bf16)
    named = jnp.moveaxis(named, 0, 1).reshape(rows, layers * all_experts)
    named = jnp.pad(named, ((0, 0), (0, lanes - layers * all_experts)))

    def normed(values, gain):
        scale = rms_scale(values)
        return scale, (values * scale * gain).astype(bf16)

    current = inputs.astype(f32)
    scale_one, normed_one = normed(current, attention_gain[0])
    gathered, named_all, *weights_now = transfer(
        "enter",
        1,
        [lambda: Gather("head"), lambda: Spread()] + weight_tasks(),
        [normed_one, named] + weight_pieces(0),
    )
    named_all = named_all.reshape(group, lanes)
    earlier = (
        jnp.arange(group, dtype=jnp.int32)[:, None] < jnp.arange(group, dtype=jnp.int32)[None, :]
    ).astype(bf16)
    rank = dot(named_all, earlier, ((0,), (0,)))
    named_t = named_all.astype(f32).T
    slots = jnp.arange(capacity, dtype=jnp.int32).astype(f32)

    def routing(layer):
        base = layer * all_experts
        hits = named_t[base : base + all_experts] > 0
        local_rank = lax.dynamic_slice_in_dim(
            rank[base : base + all_experts], first_expert, per_core, 0
        )
        local_hit = lax.dynamic_slice_in_dim(
            named_t[base : base + all_experts], first_expert, per_core, 0
        )
        slot = jnp.where(local_hit > 0, local_rank, -1.0)
        chosen = (slot[:, None, :] == slots[None, :, None]).astype(bf16)
        return hits, chosen

    def local_part(weights):
        return lax.dynamic_slice_in_dim(weights, core * per_core, per_core, 0)

    def to_homes(name, partial):
        blocks = partial.astype(bf16).reshape(cores, owners, rows, width)
        (other,) = transfer(name + "_core", 2, [lambda: Swap()], [blocks])
        mine = lax.dynamic_index_in_dim(blocks, core, 0, keepdims=False)
        both = (mine.astype(f32) + other.astype(f32)).astype(bf16)
        (parts,) = transfer(name + "_owner", 3, [lambda: Exchange("expert")], [both])
        return parts.astype(f32).sum(axis=0)

    def over_heads(blocks):
        if heads_axis != 4:
            return lax.psum_scatter(blocks, "head", scatter_dimension=0, tiled=True)[0]
        square = blocks.reshape(2, 2, *blocks.shape[1:])
        spot = {0: place // 2, 1: place % 2}
        done = []
        for half, order in zip(jnp.split(square, [per_core // 2], axis=2), ((1, 0), (0, 1))):
            for step, dim in enumerate(order):
                pairs = [(i, i ^ (2 - dim)) for i in range(4)]
                at = dim if step == 0 else 0
                away = lax.dynamic_index_in_dim(half, 1 - spot[dim], at, keepdims=False)
                here = lax.dynamic_index_in_dim(half, spot[dim], at, keepdims=False)
                came = lax.ppermute(away, "head", pairs)
                half = (here.astype(f32) + came.astype(f32)).astype(bf16)
            done.append(half)
        return jnp.concatenate(done, axis=0)

    saved = []
    for layer in range(layers):
        weight_qkv, weight_o = whole_weights(weights_now)
        own_rows = gathered.reshape(half_len, width)
        lin = dot(own_rows, weight_qkv, ((1,), (0,)))
        queries = rotate(
            lin[:, :q_width].reshape(half_len, q_heads, head_dim), cos_own, sin_own, 1.0
        ).astype(bf16)
        own_keys = rotate(
            lin[:, q_width : q_width + kv_width].reshape(half_len, kv_heads, head_dim),
            cos_own,
            sin_own,
            1.0,
        ).astype(bf16)
        own_kv = jnp.concatenate(
            [own_keys.reshape(half_len, kv_width), lin[:, q_width + kv_width :].astype(bf16)],
            axis=1,
        )
        (both_kv,) = transfer("keys", 4, [lambda: Gather("dp")], [own_kv])
        both_kv = both_kv.reshape(length, 2 * kv_width)
        keys = both_kv[:, :kv_width].reshape(length, kv_heads, head_dim)
        values = both_kv[:, kv_width:].reshape(length, kv_heads, head_dim)
        grouped = queries.reshape(half_len, kv_heads, share, head_dim)
        scores = jnp.einsum("qcgd,kcd->cgqk", grouped, keys, preferred_element_type=f32) * factor
        scores = jnp.where(mask[None, None], scores, NEG)
        peak = jnp.max(scores, axis=-1, keepdims=True)
        raised = jnp.exp(scores - peak)
        total = jnp.sum(raised, axis=-1, keepdims=True)
        probs = (raised / total).astype(bf16)
        heads_flat = (
            jnp.einsum("cgqk,kcd->qcgd", probs, values, preferred_element_type=f32)
            .astype(bf16)
            .reshape(half_len, q_width)
        )
        log_total = peak + jnp.log(total)
        partial = dot(heads_flat, weight_o, ((1,), (0,))).astype(bf16)
        tasks, operands = [lambda: Exchange("head")], [partial.reshape(heads_axis, rows, width)]
        if layer + 1 < layers:
            tasks, operands = tasks + weight_tasks(), operands + weight_pieces(layer + 1)
        parts, *weights_next = transfer(f"attended_{layer}", 5 + layer, tasks, operands)
        middle = current + parts.astype(f32).sum(axis=0)
        scale_two, normed_two = normed(middle, mixture_gain[layer])
        (tokens,) = transfer("tokens", 10, [lambda: Spread()], [normed_two])
        tokens = tokens.reshape(group, width)
        hits, chosen = routing(layer)
        logits = dot(router_weight[layer], tokens, ((0,), (1,)))
        logits = jnp.where(hits, logits, NEG)
        lifted = jnp.where(hits, jnp.exp(logits - jnp.max(logits, axis=0, keepdims=True)), 0.0)
        gates = lifted / jnp.sum(lifted, axis=0, keepdims=True)
        own_gates = lax.dynamic_slice_in_dim(gates, first_expert, per_core, 0)
        received = jnp.einsum("jst,td->jsd", chosen, tokens, preferred_element_type=f32).astype(
            bf16
        )
        w_in, w_out = local_part(expert_in[layer]), local_part(expert_out[layer])
        mixed = jnp.einsum("jsd,jdf->jsf", received, w_in, preferred_element_type=f32)
        gate_part, up_part = mixed[..., :hidden_width], mixed[..., hidden_width:]
        hidden = (jax.nn.silu(gate_part) * up_part).astype(bf16)
        expert_y = jnp.einsum("jsf,jfd->jsd", hidden, w_out, preferred_element_type=f32).astype(
            bf16
        )
        weighted = (chosen.astype(f32) * own_gates[:, None, :]).astype(bf16)
        mixture = to_homes(
            "mixture",
            dot(
                weighted.reshape(per_core * capacity, group),
                expert_y.reshape(per_core * capacity, width),
                ((0,), (0,)),
            ),
        )
        saved.append(
            (
                current,
                scale_one,
                own_rows,
                weight_qkv,
                weight_o,
                grouped,
                keys,
                values,
                heads_flat,
                log_total,
                middle,
                scale_two,
                chosen,
                own_gates,
                received,
                gate_part,
                up_part,
                hidden,
                expert_y,
                mixture,
                w_in,
                w_out,
            )
        )
        current = middle + mixture
        if layer + 1 < layers:
            scale_one, normed_one = normed(current, attention_gain[layer + 1])
            (gathered,) = transfer("rows", 11, [lambda: Gather("head")], [normed_one])
            weights_now = weights_next
    outputs = current.astype(bf16)

    grad = cotangent.astype(f32)
    gains_a, gains_m, routers = [None] * layers, [None] * layers, [None] * layers
    qkv_grads, out_grads = [None] * layers, [None] * layers
    in_grads, down_grads = [None] * layers, [None] * layers
    for layer in reversed(range(layers)):
        (
            state_in,
            scale_one,
            own_rows,
            weight_qkv,
            weight_o,
            grouped,
            keys,
            values,
            heads_flat,
            log_total,
            middle,
            scale_two,
            chosen,
            own_gates,
            received,
            gate_part,
            up_part,
            hidden,
            expert_y,
            mixture,
            w_in,
            w_out,
        ) = saved[layer]
        grad_low = grad.astype(bf16)
        inner = jnp.sum(grad_low.astype(f32) * mixture, axis=1)[None, :]
        grads, inners = transfer(
            "grads", 12, [lambda: Spread(), lambda: Spread()], [grad_low, inner]
        )
        grads, inners = grads.reshape(group, width), inners.reshape(group)
        chosen_f = chosen.astype(f32)
        row_gates = jnp.sum(chosen_f * own_gates[:, None, :], axis=-1, keepdims=True)
        row_inner = jnp.sum(chosen_f * inners[None, None, :], axis=-1, keepdims=True)
        row_grads = jnp.einsum("jst,td->jsd", chosen, grads, preferred_element_type=f32)
        row_dgates = jnp.sum(row_grads * expert_y.astype(f32), axis=-1, keepdims=True)
        dy = (row_gates * row_grads).astype(bf16)
        dz = row_gates * (row_dgates - row_inner)
        dhidden = jnp.einsum("jsd,jfd->jsf", dy, w_out, preferred_element_type=f32)
        sigma = jax.nn.sigmoid(gate_part)
        dgate = dhidden * up_part * sigma * (1.0 + gate_part * (1.0 - sigma))
        dup = dhidden * (gate_part * sigma)
        dmixed = jnp.concatenate([dgate, dup], axis=-1).astype(bf16)
        router_rows = lax.dynamic_slice_in_dim(
            router_weight[layer].T, first_expert, per_core, 0
        ).astype(f32)
        drow = jnp.einsum("jsf,jdf->jsd", dmixed, w_in, preferred_element_type=f32)
        drow = (drow + dz * router_rows[:, None, :]).astype(bf16)
        routers[layer] = jnp.sum(received.astype(f32) * dz, axis=1)
        dnormed_two = to_homes(
            "dtokens",
            dot(
                chosen.reshape(per_core * capacity, group),
                drow.reshape(per_core * capacity, width),
                ((0,), (0,)),
            ),
        )
        grad_in = jnp.einsum(
            "jspha,jsf->hjpaf",
            received.reshape(per_core, capacity, cores, heads_axis, -1),
            dmixed,
            preferred_element_type=f32,
        ).astype(bf16)
        grad_down = jnp.einsum(
            "jspha,jsd->hjpad",
            hidden.reshape(per_core, capacity, cores, heads_axis, -1),
            dy,
            preferred_element_type=f32,
        ).astype(bf16)
        in_grads[layer] = over_heads(grad_in)
        down_grads[layer] = over_heads(grad_down)
        dmiddle, gains_m[layer] = norm_back(middle, scale_two, mixture_gain[layer], dnormed_two)
        dmiddle = grad + dmiddle
        (full_dattn,) = transfer("dattn", 11, [lambda: Gather("head")], [dmiddle.astype(bf16)])
        full_dattn = full_dattn.reshape(half_len, width)
        grad_o = dot(heads_flat, full_dattn, ((0,), (0,))).astype(bf16)
        dheads = dot(full_dattn, weight_o, ((1,), (1,))).astype(bf16)
        dgrouped = dheads.reshape(half_len, kv_heads, share, head_dim)
        scores = jnp.einsum("qcgd,kcd->cgqk", grouped, keys, preferred_element_type=f32) * factor
        scores = jnp.where(mask[None, None], scores, NEG)
        probs = jnp.exp(scores - log_total)
        dprobs = jnp.einsum("qcgd,kcd->cgqk", dgrouped, values, preferred_element_type=f32)
        delta = jnp.sum(probs * dprobs, axis=-1, keepdims=True)
        dscores = (probs * (dprobs - delta)).astype(bf16)
        dqueries = jnp.einsum("cgqk,kcd->qcgd", dscores, keys, preferred_element_type=f32) * factor
        dkeys = jnp.einsum("cgqk,qcgd->kcd", dscores, grouped, preferred_element_type=f32) * factor
        dvalues = jnp.einsum(
            "cgqk,qcgd->kcd", probs.astype(bf16), dgrouped, preferred_element_type=f32
        )
        dkv = jnp.concatenate(
            [dkeys.reshape(length, kv_width), dvalues.reshape(length, kv_width)], axis=1
        ).reshape(cores, half_len, 2 * kv_width)
        (dkv_other,) = transfer("dkeys", 13, [lambda: Swap()], [dkv.astype(bf16)])
        dkv = lax.dynamic_index_in_dim(dkv, core, 0, keepdims=False) + dkv_other.astype(f32)
        dq_lin = rotate(
            dqueries.reshape(half_len, q_heads, head_dim), cos_own, sin_own, -1.0
        ).reshape(half_len, q_width)
        dk_lin = rotate(
            dkv[:, :kv_width].reshape(half_len, kv_heads, head_dim), cos_own, sin_own, -1.0
        ).reshape(half_len, kv_width)
        dlin = jnp.concatenate([dq_lin, dk_lin, dkv[:, kv_width:]], axis=1).astype(bf16)
        grad_qkv = dot(own_rows, dlin, ((0,), (0,))).astype(bf16)
        part = dot(dlin, weight_qkv, ((1,), (1,))).astype(bf16)
        grad_qkv = grad_qkv.reshape(cores, owners, -1, wide)
        grad_o = jnp.moveaxis(grad_o.reshape(out_rows, cores, owners, -1), 0, 2)
        parts, qkv_other, out_other = transfer(
            "dlin",
            14,
            [lambda: Exchange("head"), lambda: Swap(), lambda: Swap()],
            [part.reshape(heads_axis, rows, width), grad_qkv, grad_o],
        )

        def with_other(blocks, other):
            mine = lax.dynamic_index_in_dim(blocks, core, 0, keepdims=False)
            return (mine.astype(f32) + other.astype(f32)).astype(bf16)

        qkv_parts, out_parts = transfer(
            "weight_grads",
            15,
            [lambda: Exchange("expert"), lambda: Exchange("expert")],
            [with_other(grad_qkv, qkv_other), with_other(grad_o, out_other)],
        )
        qkv_grads[layer] = qkv_parts.astype(f32).sum(axis=0)
        out_grads[layer] = out_parts.astype(f32).sum(axis=0)
        dnormed_one = parts.astype(f32).sum(axis=0)
        dstate, gains_a[layer] = norm_back(
            state_in, scale_one, attention_gain[layer], dnormed_one
        )
        grad = dmiddle + dstate

    def own_slices(pieces):
        other = lax.dynamic_index_in_dim(pieces, 1 - core, 1, keepdims=False)
        mine = lax.dynamic_index_in_dim(pieces, core, 1, keepdims=False)
        swapped = lax.ppermute(other, "dp", [(0, 1), (1, 0)])
        both = jnp.stack([mine, swapped])
        first = lax.dynamic_index_in_dim(both, core, 0, keepdims=False)
        second = lax.dynamic_index_in_dim(both, 1 - core, 0, keepdims=False)
        return jnp.concatenate([first, second], axis=0).astype(f32)

    small = jnp.concatenate(routers + [jnp.stack(gains_a), jnp.stack(gains_m)], axis=0)
    (small,) = transfer("small_head", 16, [lambda: Gather("head")], [small])
    (small,) = transfer("small_group", 17, [lambda: Spread()], [small.sum(axis=0)])
    from_experts = layers * per_core
    router_grad = (
        small[:, :, :from_experts]
        .reshape(cores, owners, layers, per_core, width)
        .transpose(2, 4, 1, 0, 3)
        .reshape(layers, width, all_experts)
    )
    gains = small[:, :, from_experts:].sum(axis=(0, 1))
    qkv_grad = jnp.stack(qkv_grads)
    return (
        outputs,
        grad,
        gains[:layers],
        gains[layers:],
        qkv_grad[..., :q_width],
        qkv_grad[..., q_width : q_width + kv_width],
        qkv_grad[..., q_width + kv_width :],
        jnp.stack(out_grads),
        router_grad,
        jnp.stack([own_slices(p) for p in in_grads]),
        jnp.stack([own_slices(p) for p in down_grads]),
    )


def solution(mesh):
    plan = per_device_dense if token_plan_fits(mesh) else per_device_rows
    in_specs = (
        P(("dp", "expert", "head"), None),
        P(("dp", "expert", "head"), None),
        P("expert", None),
        P(None, ("dp", "expert", "head"), None),
        P(),
        P(),
        P(None, "expert", "head"),
        P(None, "expert", "head"),
        P(None, "expert", "head"),
        P(None, "head", "expert"),
        P(),
        P(None, "expert", None, None),
        P(None, "expert", None, None),
    )
    out_specs = (
        P(("dp", "expert", "head"), None),
        P(("dp", "expert", "head"), None),
        P(),
        P(),
        P(None, ("dp", "expert"), "head"),
        P(None, ("dp", "expert"), "head"),
        P(None, ("dp", "expert"), "head"),
        P(None, "head", ("dp", "expert")),
        P(),
        P(None, "expert", ("dp", "head"), None),
        P(None, "expert", ("dp", "head"), None),
    )
    return jax.shard_map(
        plan, mesh=mesh, in_specs=in_specs, out_specs=out_specs, check_vma=False
    )
```
